32 devices in a mesh: rows: 8 (over y, x, core), grp: 4 (over z).
Axes of the slice: x: 2, y: 2, z: 4, core: 2. Of those that a mesh axis runs over, the one named last changes fastest.
Arguments:
- matrix: bfloat16 [16384, 2048], P(('rows', 'grp')), may hold values from -0.09375 to 0.09375
- right_side: bfloat16 [16384, 128], P(('rows', 'grp')), may hold values from -6 to 6
- precond: bfloat16 [2048, 2048], replicated, may hold values from -1 to 3
- row_counts: int32 [32], P(('rows', 'grp')), may hold values from 64 to 512, as said below
Outputs:
- solution: float32 [2048, 128], P(None, 'grp')
- coeffs: float32 [2048, 128], P(None, 'grp')
- rel_residual: float32 [128], P('grp')
The draws below stay inside these ranges and needn't reach their ends.
Inputs may be any that keep to these rules, and one draw needn't show every extreme that they name: Device d holds A's rows in its first row_counts[d] slots of 512; some device is full in every draw.
All inputs are finite; a program needn't handle non-finite values.
Results may differ from the reference program's by a relative error of at most 0.0128.
Values may be sent and summed in bfloat16 or wider, within the bound.
A program may use at most 64 MiB of HBM per device.

```python
import math
import jax
import jax.numpy as jnp
from jax import lax

D = 2048
K = 128
ITERS = 3
R_DEV = 512
NDEV = 32
ROWS = 16384


def draw_row_counts(key, part):
    first, second = jax.random.split(key)
    base = jax.random.randint(first, (NDEV,), R_DEV // 8, R_DEV // 2 + 1, dtype=jnp.int32)
    fullest = jax.random.randint(second, (), 0, NDEV, dtype=jnp.int32)
    return jnp.where(jnp.arange(NDEV, dtype=jnp.int32) == fullest, R_DEV, base).astype(jnp.int32)


def draw_precond(key, part):
    first, second = jax.random.split(key)
    scales = jnp.exp(jax.random.uniform(first, (D,), minval=math.log(0.25), maxval=math.log(2.0)))
    noise = jax.random.normal(second, (D, D))
    return (jnp.diag(scales) + 0.5 * noise / math.sqrt(D)).astype(jnp.bfloat16)


def strengthened(values, stream_key, source, target, blocks, factor):
    def block_of(dim):
        return (jnp.arange(values.shape[dim]) // (values.shape[dim] // blocks)).reshape((-1,) + (1,) * (values.ndim - 1 - dim))

    near = jax.random.permutation(stream_key, blocks)[block_of(target)]
    second = (block_of(target) + blocks // 2) % blocks
    return jnp.where((block_of(source) == near) | (block_of(source) == second), factor * values, values)


def shard_levels(own_key, dims, shards, smallest, largest):
    def one(axis_at, blocks):
        steps = jax.random.uniform(jax.random.fold_in(jax.random.fold_in(own_key, 6), axis_at), (blocks,), jnp.float32, smallest / len(shards), largest / len(shards))
        return jnp.repeat(jnp.exp(steps), dims[axis_at] // blocks).reshape((-1,) + (1,) * (len(dims) - axis_at - 1))

    loudness = one(*shards[0])
    for cut in shards[1:]:
        loudness = loudness * one(*cut)
    return loudness


def normal_values(key, extent, width, reach, cuts=(), kind=jnp.bfloat16):
    loudness = shard_levels(key, extent, cuts, -0.22, 0.18) if cuts else 1.0
    values = jax.random.normal(key, extent, jnp.float32) * width * loudness
    return jnp.minimum(jnp.maximum(values, -reach), reach).astype(kind)


def noise_with(own_key, dims, width, reach, shards, heavy, kind=jnp.bfloat16):
    result = width * jax.random.normal(own_key, dims, jnp.float32)
    if shards:
        result = result * shard_levels(own_key, dims, shards, -0.22, 0.18)
    return jnp.clip(strengthened(result, jax.random.fold_in(own_key, 3), *heavy), -reach, reach).astype(kind)


def setup_inputs(seed: int = 0) -> dict:
    key_list = jax.random.split(jax.random.key(seed), 5)
    return {
        "matrix": noise_with(key_list[0], (ROWS, D), ROWS ** -0.5, 0.09375, ((0, 32),), (0, 1, 32, 2.75)),
        "right_side": normal_values(key_list[1], (ROWS, K), 1.0, 6.0, ((0, 32),)),
        "precond": draw_precond(jax.random.fold_in(key_list[4], 71), 0),
        "row_counts": draw_row_counts(jax.random.fold_in(key_list[4], 71), 0),
    }


floor_sq = 0.01

def pull_back(matrix, precond, residue):
    partial_value = lax.dot_general(matrix, residue.astype(jnp.bfloat16), (((0,), (0,)), ((), ())), preferred_element_type=jnp.float32)
    squares = lax.optimization_barrier(jnp.sum(residue * residue, axis=0, keepdims=True))
    u_norm = jnp.sqrt(squares + floor_sq)
    pulled = lax.dot_general(precond, (partial_value / u_norm).astype(jnp.bfloat16), (((0,), (0,)), ((), ())), preferred_element_type=jnp.float32)
    return (u_norm, pulled)

def reference(matrix, right_side, precond, row_counts):
    total_rows = matrix.shape[0]
    position = jnp.arange(total_rows, dtype=jnp.int32)
    owner = (position // R_DEV).astype(jnp.int32)
    live_rows = (position % R_DEV < row_counts[owner]).astype(jnp.float32)[:, None]
    residue = live_rows * right_side.astype(jnp.float32)
    u_norm, pulled = pull_back(matrix, precond, residue)
    v_norm = jnp.sqrt(lax.optimization_barrier(jnp.sum(pulled * pulled, axis=0, keepdims=True)) + floor_sq)
    right_vec = pulled / v_norm
    left_vec = residue / u_norm
    phi_bar = u_norm
    rho_bar = v_norm
    search = right_vec
    coeffs = jnp.zeros(right_vec.shape, jnp.float32)
    start_norm = u_norm
    for turn_index in range(ITERS):
        pushed = jnp.dot(precond, right_vec.astype(jnp.bfloat16), preferred_element_type=jnp.float32).astype(jnp.bfloat16)
        residue = live_rows * (jnp.dot(matrix, pushed, preferred_element_type=jnp.float32) - v_norm * left_vec)
        u_norm, pulled = pull_back(matrix, precond, residue)
        raw_vec = pulled - u_norm * right_vec
        next_norm = jnp.sqrt(lax.optimization_barrier(jnp.sum(raw_vec * raw_vec, axis=0, keepdims=True)) + floor_sq)
        next_vec = raw_vec / next_norm
        left_vec = residue / u_norm
        radius = jnp.sqrt(rho_bar * rho_bar + u_norm * u_norm)
        cosine = rho_bar / radius
        sine_part = u_norm / radius
        coupling = sine_part * next_norm
        rho_bar = -cosine * next_norm
        phi_step = cosine * phi_bar
        phi_bar = sine_part * phi_bar
        coeffs = coeffs + phi_step / radius * search
        search = next_vec - coupling / radius * search
        right_vec = next_vec
        v_norm = next_norm
    solution = jnp.dot(precond, coeffs.astype(jnp.bfloat16), preferred_element_type=jnp.float32)
    return (solution, coeffs, (phi_bar / start_norm)[0])
```

```python
import functools

import jax
import jax.numpy as jnp
from jax import lax
from jax.experimental import pallas as pl
from jax.experimental.pallas import tpu as pltpu
from jax.sharding import PartitionSpec as P

ITERS = 3
CORES = 2
FLOOR_SQ = 0.01
F32 = jnp.float32
BF16 = jnp.bfloat16
MESH = pl.DeviceIdType.MESH


def body(
    nxy, nz,
    count_ref, a_hbm, b_ref, n_hbm,
    sol_ref, coef_ref, ratio_ref,
    a_ref, n_ref, c_ref, ct_ref, left_ref, vecs_ref, pb_ref, vb_ref, ft_ref, w_ref, nw_ref,
    tx0, rx0, hbuf, tx1, rx1, tx2, rx2, full,
    sqtx, sqrx0, sqrx1, sqrx2,
    load_sem, s0, r0, s1, r1, s2, r2, gs2, gr2, gs1, gr1, gs0, gr0,
    qs0, qr0, qs1, qr1, qs2, qr2,
):
    row = lax.axis_index("rows")
    z = lax.axis_index("grp")
    core = lax.rem(row, CORES)
    xy = row // CORES
    other = 1 - core
    local, width = a_ref.shape
    cols = b_ref.shape[1]
    chunk = full.shape[3]
    group = nxy * chunk
    own_cols = cols // nz

    def xy_peer(k):
        return lax.rem(xy + k, nxy)

    def z_peer(k):
        return lax.rem(z + k, nz)

    def row_id(at):
        return {"rows": at * CORES + core}

    core_id = {"rows": xy * CORES + other}

    load_a = pltpu.make_async_copy(a_hbm, a_ref, load_sem.at[0])
    load_n = pltpu.make_async_copy(n_hbm, n_ref, load_sem.at[1])
    load_a.start()
    load_n.start()

    barrier = pltpu.get_barrier_semaphore()
    pl.semaphore_signal(barrier, inc=1, device_id=core_id, device_id_type=MESH)
    for k in range(1, nxy):
        pl.semaphore_signal(barrier, inc=1, device_id=row_id(xy_peer(k)), device_id_type=MESH)
    for k in range(1, nz):
        pl.semaphore_signal(barrier, inc=1, device_id={"grp": z_peer(k)}, device_id_type=MESH)

    def remote(src, dst, ssem, rsem, to):
        copy = pltpu.make_async_remote_copy(
            src_ref=src, dst_ref=dst, send_sem=ssem, recv_sem=rsem, device_id=to, device_id_type=MESH
        )
        copy.start()
        return copy

    def flat(value):
        return value.astype(F32).reshape(-1, cols)

    def pieces(value):
        return value.reshape(-1, chunk, cols).astype(BF16)

    class Squares:
        def __init__(self, turn, local_sq):
            self.turn = turn
            self.total = jnp.broadcast_to(local_sq, (8, cols))
            self.sent = []

        def send_core(self):
            sqtx[self.turn, 0] = self.total
            self.now = [remote(sqtx.at[self.turn, 0], sqrx0.at[self.turn], qs0.at[self.turn], qr0.at[self.turn], core_id)]

        def send_xy(self):
            self.now[0].wait_recv()
            self.sent += self.now
            self.total = self.total + sqrx0[self.turn]
            sqtx[self.turn, 1] = self.total
            sqrx1[self.turn, xy] = self.total
            self.now = [
                remote(sqtx.at[self.turn, 1], sqrx1.at[self.turn, xy], qs1.at[self.turn, k - 1], qr1.at[self.turn, k - 1], row_id(xy_peer(k)))
                for k in range(1, nxy)
            ]

        def send_z(self):
            for copy in self.now:
                copy.wait_recv()
            self.sent += self.now
            self.total = sum(sqrx1[self.turn, at] for at in range(nxy))
            sqtx[self.turn, 2] = self.total
            sqrx2[self.turn, z] = self.total
            self.now = [
                remote(sqtx.at[self.turn, 2], sqrx2.at[self.turn, z], qs2.at[self.turn, k - 1], qr2.at[self.turn, k - 1], {"grp": z_peer(k)})
                for k in range(1, nz)
            ]

        def finish(self):
            for copy in self.now:
                copy.wait_recv()
            self.sent += self.now
            self.total = sum(sqrx2[self.turn, at] for at in range(nz))
            for copy in self.sent:
                copy.wait_send()
            return self.total[0:1]

    def all_reduce(turn, product, local_sq, filler):
        order = list(range(1, nz)) + [0]
        sends = []
        core_copies = {}
        for d in order:
            s = z_peer(d)
            tx0[s] = pieces(product(other, s))
            core_copies[d] = remote(tx0.at[s], rx0.at[s], s0.at[d], r0.at[d], core_id)
        squares = Squares(turn, local_sq)
        squares.send_core()
        for d in order:
            s = z_peer(d)
            hbuf[s] = product(core, s).reshape(nxy, chunk, cols)
        xy_copies = {}
        for d in order:
            s = z_peer(d)
            core_copies[d].wait_recv()
            total = hbuf[s] + rx0[s].astype(F32)
            hbuf[s] = total
            tx1[s] = total.astype(BF16)
            for k in range(1, nxy):
                at = xy_peer(k)
                xy_copies[d, k] = remote(
                    tx1.at[s, at], rx1.at[d, k - 1], s1.at[d, k - 1], r1.at[d, k - 1], row_id(at)
                )
        squares.send_xy()
        filler(2)
        z_copies = {}
        for d in order:
            s = z_peer(d)
            part = hbuf[s, xy]
            for k in range(1, nxy):
                xy_copies[d, k].wait_recv()
                part = part + rx1[d, k - 1].astype(F32)
            if d:
                tx2[d - 1] = part.astype(BF16)
                z_copies[d] = remote(
                    tx2.at[d - 1], rx2.at[d - 1], s2.at[d - 1], r2.at[d - 1], {"grp": s}
                )
        squares.send_z()
        filler(2)
        for d in range(1, nz):
            z_copies[d].wait_recv()
            part = part + rx2[d - 1].astype(F32)
        full[core, z, xy] = part.astype(BF16)
        gather_z = [
            remote(full.at[core, z, xy], full.at[core, z, xy], gs2.at[d - 1], gr2.at[d - 1], {"grp": z_peer(d)})
            for d in range(1, nz)
        ]
        gather_xy = {}

        def spread(d, zz):
            for k in range(1, nxy):
                gather_xy[d, k] = remote(
                    full.at[core, zz, xy], full.at[core, zz, xy],
                    gs1.at[d, k - 1], gr1.at[d, k - 1], row_id(xy_peer(k)),
                )

        spread(0, z)
        total_sq = squares.finish()
        filler(3)
        for d in range(1, nz):
            gather_z[d - 1].wait_recv()
            spread(d, z_peer(nz - d))
        filler(1)
        gather_core = []
        for d in range(nz):
            zz = z_peer((nz - d) % nz)
            for k in range(1, nxy):
                gather_xy[d, k].wait_recv()
            gather_core.append(
                remote(full.at[core, zz], full.at[core, zz], gs0.at[d], gr0.at[d], core_id)
            )
        for copy in gather_core:
            copy.wait_recv()
        for copies in (core_copies, xy_copies, z_copies, gather_xy):
            for copy in copies.values():
                copy.wait_send()
        for copy in gather_z + gather_core:
            copy.wait_send()
        return total_sq

    live = (lax.broadcasted_iota(jnp.int32, (local, 1), 0) < count_ref[0]).astype(F32)

    residue = live * b_ref[...].astype(F32)
    left_ref[...] = residue
    sq = jnp.sum(residue * residue, axis=0, keepdims=True)
    bt = residue.T.astype(BF16)
    pl.semaphore_wait(barrier, nxy + nz - 1)
    load_a.wait()

    def first_product(half, s):
        start = pl.multiple_of((half * nz + s) * group, group)
        return jnp.dot(bt, a_ref[:, pl.ds(start, group)], preferred_element_type=F32).T

    block = 256
    todo = list(range(width // block))

    def form_c(times):
        if len(todo) == width // block:
            load_n.wait()
        for _ in range(times):
            if todo:
                at = todo.pop(0) * block
                value = live * jnp.dot(a_ref[...], n_ref[:, at : at + block], preferred_element_type=F32)
                c_ref[:, at : at + block] = value.astype(BF16)
                ct_ref[at : at + block, :] = value.T.astype(BF16)

    def later_product(half, s):
        start = pl.multiple_of((half * nz + s) * group, group)
        return jnp.dot(ct_ref[pl.ds(start, group), :], pb_ref[...], preferred_element_type=F32)

    groups = [(h, s) for h in range(CORES) for s in range(nz)]

    def rows_of(h, s):
        at = (h * nz + s) * group
        return slice(at, at + group)

    u_norm = jnp.sqrt(all_reduce(0, first_product, sq, form_c) + FLOOR_SQ)
    form_c(len(todo))
    for h, s in groups:
        ft_ref[:, rows_of(h, s)] = flat(full[h, s]).T.astype(BF16)
    inverse = 1.0 / u_norm
    total = jnp.zeros((1, cols), F32)
    for at in range(0, width, block):
        raw = jnp.dot(ft_ref[...], n_ref[:, at : at + block], preferred_element_type=F32).T * inverse
        vecs_ref[0, at : at + block] = raw
        total = total + jnp.sum(raw * raw, axis=0, keepdims=True)
    v_norm = jnp.sqrt(total + FLOOR_SQ)

    def normalise(at_vec, norm):
        scale = 1.0 / norm
        for at in range(0, width, block):
            value = vecs_ref[at_vec, at : at + block] * scale
            vecs_ref[at_vec, at : at + block] = value
            vb_ref[at : at + block] = value.astype(BF16)

    normalise(0, v_norm)
    phi_bar = u_norm
    rho_bar = v_norm
    start_norm = u_norm
    search = [jnp.ones((1, cols), F32)]
    coeffs = [jnp.zeros((1, cols), F32)]

    def project(v_norm, u_norm):
        residue = jnp.dot(c_ref[...], vb_ref[...], preferred_element_type=F32) - left_ref[...] * (v_norm / u_norm)
        left_ref[...] = residue
        pb_ref[...] = residue.astype(BF16)
        return jnp.sum(residue * residue, axis=0, keepdims=True)

    for turn in range(ITERS - 1):
        sq = project(v_norm, u_norm)
        u_norm = jnp.sqrt(all_reduce(turn + 1, later_product, sq, lambda times: None) + FLOOR_SQ)
        inverse = 1.0 / u_norm
        total = jnp.zeros((1, cols), F32)
        for h, s in groups:
            raw = flat(full[h, s]) * inverse - u_norm * vecs_ref[turn, rows_of(h, s)]
            vecs_ref[turn + 1, rows_of(h, s)] = raw
            total = total + jnp.sum(raw * raw, axis=0, keepdims=True)
        v_norm = jnp.sqrt(total + FLOOR_SQ)
        normalise(turn + 1, v_norm)
        radius = jnp.sqrt(rho_bar * rho_bar + u_norm * u_norm)
        cosine = rho_bar / radius
        sine = u_norm / radius
        coupling = sine * v_norm
        rho_bar = -cosine * v_norm
        step = cosine * phi_bar / radius
        phi_bar = sine * phi_bar
        coeffs = [c + step * p for c, p in zip(coeffs, search)] + [jnp.zeros((1, cols), F32)]
        search = [-(coupling / radius) * p for p in search] + [jnp.ones((1, cols), F32)]

    squares = Squares(ITERS, project(v_norm, u_norm))
    squares.send_core()
    shift = lax.rem(cols - z * own_cols, cols)
    for at in range(0, width, block):
        known = sum(c * vecs_ref[i, at : at + block] for i, c in enumerate(coeffs))
        along = sum(p * vecs_ref[i, at : at + block] for i, p in enumerate(search))
        known = pltpu.roll(known, shift, 1)
        along = pltpu.roll(along, shift, 1)
        vecs_ref[0, at : at + block] = known
        vecs_ref[1, at : at + block] = along
        w_ref[at : at + block, :cols] = known.astype(BF16)
        w_ref[at : at + block, cols:] = along.astype(BF16)

    def form_solution(first, last):
        for at in range(first, last, block):
            nw_ref[at : at + block] = jnp.dot(
                n_ref[at : at + block, :], w_ref[...], preferred_element_type=F32
            )

    squares.send_xy()
    form_solution(0, width // 2)
    squares.send_z()
    form_solution(width // 2, width)
    u_norm = jnp.sqrt(squares.finish() + FLOOR_SQ)
    radius = jnp.sqrt(rho_bar * rho_bar + u_norm * u_norm)
    step = rho_bar / radius * phi_bar / radius
    ratio = u_norm / radius * phi_bar / start_norm
    step = pltpu.roll(jnp.broadcast_to(step, (8, cols)), shift, 1)[0:1]
    ratio_ref[...] = pltpu.roll(jnp.broadcast_to(ratio, (8, cols)), shift, 1)[0:1, :own_cols]
    for at in range(0, width, block):
        coef_ref[at : at + block] = (vecs_ref[0, at : at + block] + step * vecs_ref[1, at : at + block])[:, :own_cols]
        sol_ref[at : at + block] = (
            nw_ref[at : at + block, :cols] + step * nw_ref[at : at + block, cols:]
        )[:, :own_cols]


def shards(nrows, nz, matrix, right_side, precond, row_counts):
    local, width = matrix.shape
    cols = right_side.shape[1]
    nxy = nrows // CORES
    chunk = width // (nrows * nz)
    own = cols // nz
    turns = ITERS + 1
    vmem = pltpu.VMEM
    dma = pltpu.SemaphoreType.DMA
    sol, coef, ratio = pl.pallas_call(
        functools.partial(body, nxy, nz),
        out_shape=(
            jax.ShapeDtypeStruct((width, own), F32),
            jax.ShapeDtypeStruct((width, own), F32),
            jax.ShapeDtypeStruct((1, own), F32),
        ),
        in_specs=[
            pl.BlockSpec(memory_space=pltpu.SMEM),
            pl.BlockSpec(memory_space=pl.ANY),
            pl.BlockSpec(memory_space=vmem),
            pl.BlockSpec(memory_space=pl.ANY),
        ],
        out_specs=[pl.BlockSpec(memory_space=vmem)] * 3,
        scratch_shapes=[
            vmem((local, width), BF16),
            vmem((width, width), BF16),
            vmem((local, width), BF16),
            vmem((width, local), BF16),
            vmem((local, cols), F32),
            vmem((ITERS, width, cols), F32),
            vmem((local, cols), BF16),
            vmem((width, cols), BF16),
            vmem((cols, width), BF16),
            vmem((width, 2 * cols), BF16),
            vmem((width, 2 * cols), F32),
            vmem((nz, nxy, chunk, cols), BF16),
            vmem((nz, nxy, chunk, cols), BF16),
            vmem((nz, nxy, chunk, cols), F32),
            vmem((nz, nxy, chunk, cols), BF16),
            vmem((nz, nxy - 1, chunk, cols), BF16),
            vmem((nz - 1, chunk, cols), BF16),
            vmem((nz - 1, chunk, cols), BF16),
            vmem((CORES, nz, nxy, chunk, cols), BF16),
            vmem((turns, 3, 8, cols), F32),
            vmem((turns, 8, cols), F32),
            vmem((turns, nxy, 8, cols), F32),
            vmem((turns, nz, 8, cols), F32),
            dma((2,)),
            dma((nz,)), dma((nz,)),
            dma((nz, nxy - 1)), dma((nz, nxy - 1)),
            dma((nz - 1,)), dma((nz - 1,)),
            dma((nz - 1,)), dma((nz - 1,)),
            dma((nz, nxy - 1)), dma((nz, nxy - 1)),
            dma((nz,)), dma((nz,)),
            dma((turns,)), dma((turns,)),
            dma((turns, nxy - 1)), dma((turns, nxy - 1)),
            dma((turns, nz - 1)), dma((turns, nz - 1)),
        ],
        compiler_params=pltpu.CompilerParams(
            collective_id=0, has_side_effects=True, vmem_limit_bytes=60 * 1024 * 1024
        ),
    )(row_counts, matrix, right_side, precond)
    return (sol, coef, ratio[0])


def solution(mesh):
    return jax.shard_map(
        functools.partial(shards, mesh.shape["rows"], mesh.shape["grp"]),
        mesh=mesh,
        in_specs=(P(("rows", "grp"), None), P(("rows", "grp"), None), P(), P(("rows", "grp"))),
        out_specs=(P(None, "grp"), P(None, "grp"), P("grp")),
        check_vma=False,
    )
```

```python
import functools

import jax
import jax.numpy as jnp
from jax import lax
from jax.experimental import pallas as pl
from jax.experimental.pallas import tpu as pltpu
from jax.sharding import PartitionSpec as P

ITERS = 3
CORES = 2
FLOOR_SQ = 0.01
F32 = jnp.float32
BF16 = jnp.bfloat16
MESH = pl.DeviceIdType.MESH


def body(
    nrows, nz,
    count_ref, a_hbm, b_hbm, n_hbm,
    sol_ref, coef_ref, ratio_ref,
    a_ref, b_ref, n_ref, c_ref, ct_ref, left_ref, vecs_ref, pb_ref, acc_ref, pull_ref, norms_ref,
    w_ref, flip_ref, nw_ref, step_ref,
    tx0, rx0, hbuf, tx1, rx1, tx2, rx2, full,
    sqtx, sqrx1, sqrx2,
    load_sem, s0, r0, s1, r1, s2, r2, gs2, gr2, gs1, gr1, gs0, gr0,
    qs1, qr1, qs2, qr2,
):
    row = lax.axis_index("rows")
    z = lax.axis_index("grp")
    core = lax.rem(row, CORES)
    xy = row // CORES
    other = 1 - core
    local, width = a_ref.shape
    cols = b_ref.shape[1]
    chunk = full.shape[3]
    nxy = nrows // CORES
    group = nxy * chunk
    own_cols = cols // nz

    def xy_peer(k):
        return lax.rem(xy + k, nxy)

    def z_peer(k):
        return lax.rem(z + k, nz)

    def row_id(at):
        return {"rows": at * CORES + core}

    core_id = {"rows": xy * CORES + other}

    def load_half(half, at):
        span = pl.ds(pl.multiple_of(half * (width // CORES), width // CORES), width // CORES)
        return pltpu.make_async_copy(a_hbm.at[:, span], a_ref.at[:, span], load_sem.at[at])

    load_b = pltpu.make_async_copy(b_hbm, b_ref, load_sem.at[3])
    load_other = load_half(other, 0)
    load_own = load_half(core, 1)
    load_n = pltpu.make_async_copy(n_hbm, n_ref, load_sem.at[2])
    load_b.start()
    load_other.start()
    load_own.start()
    load_n.start()

    barrier = pltpu.get_barrier_semaphore()
    for k in range(1, nrows):
        pl.semaphore_signal(barrier, inc=1, device_id={"rows": lax.rem(row + k, nrows)}, device_id_type=MESH)
    for k in range(1, nz):
        pl.semaphore_signal(barrier, inc=1, device_id={"grp": z_peer(k)}, device_id_type=MESH)

    def remote(src, dst, ssem, rsem, to):
        copy = pltpu.make_async_remote_copy(
            src_ref=src, dst_ref=dst, send_sem=ssem, recv_sem=rsem, device_id=to, device_id_type=MESH
        )
        copy.start()
        return copy

    def flat(value):
        return value.astype(F32).reshape(-1, cols)

    def pieces(value):
        return value.reshape(-1, chunk, cols).astype(BF16)

    class Squares:
        def __init__(self, turn, local_sq):
            self.turn = turn
            self.total = jnp.broadcast_to(local_sq, (8, cols))
            self.sent = []

        def send_rows(self):
            sqtx[self.turn, 0] = self.total
            sqrx1[self.turn, row] = self.total
            self.now = [
                remote(
                    sqtx.at[self.turn, 0], sqrx1.at[self.turn, row],
                    qs1.at[self.turn, k - 1], qr1.at[self.turn, k - 1],
                    {"rows": lax.rem(row + k, nrows)},
                )
                for k in range(1, nrows)
            ]

        def send_z(self):
            for copy in self.now:
                copy.wait_recv()
            self.sent += self.now
            self.total = sum(sqrx1[self.turn, at] for at in range(nrows))
            sqtx[self.turn, 1] = self.total
            sqrx2[self.turn, z] = self.total
            self.now = [
                remote(sqtx.at[self.turn, 1], sqrx2.at[self.turn, z], qs2.at[self.turn, k - 1], qr2.at[self.turn, k - 1], {"grp": z_peer(k)})
                for k in range(1, nz)
            ]

        def finish(self):
            for copy in self.now:
                copy.wait_recv()
            self.sent += self.now
            self.total = sum(sqrx2[self.turn, at] for at in range(nz))
            for copy in self.sent:
                copy.wait_send()
            return self.total[0:1]

    def all_reduce(turn, product, local_sq, filler, consume):
        order = list(range(1, nz)) + [0]
        sends = []
        core_copies = {}
        for d in order:
            s = z_peer(d)
            tx0[s] = pieces(product(other, s))
            if turn == 0 and d == order[0]:
                pl.semaphore_wait(barrier, nrows + nz - 2)
            core_copies[d] = remote(tx0.at[s], rx0.at[s], s0.at[d], r0.at[d], core_id)
        squares = Squares(turn, local_sq)
        squares.send_rows()
        if turn == 0:
            load_own.wait()
        for d in order:
            s = z_peer(d)
            hbuf[s] = product(core, s).reshape(nxy, chunk, cols)
        xy_copies = {}
        for d in order:
            s = z_peer(d)
            core_copies[d].wait_recv()
            total = hbuf[s] + rx0[s].astype(F32)
            hbuf[s] = total
            tx1[s] = total.astype(BF16)
            for k in range(1, nxy):
                at = xy_peer(k)
                xy_copies[d, k] = remote(
                    tx1.at[s, at], rx1.at[d, k - 1], s1.at[d, k - 1], r1.at[d, k - 1], row_id(at)
                )
        filler(2)
        z_copies = {}
        for d in order:
            s = z_peer(d)
            part = hbuf[s, xy]
            for k in range(1, nxy):
                xy_copies[d, k].wait_recv()
                part = part + rx1[d, k - 1].astype(F32)
            if d:
                tx2[d - 1] = part.astype(BF16)
                z_copies[d] = remote(
                    tx2.at[d - 1], rx2.at[d - 1], s2.at[d - 1], r2.at[d - 1], {"grp": s}
                )
        squares.send_z()
        filler(2)
        for d in range(1, nz):
            z_copies[d].wait_recv()
            part = part + rx2[d - 1].astype(F32)
        full[core, z, xy] = part.astype(BF16)
        gather_z = [
            remote(full.at[core, z, xy], full.at[core, z, xy], gs2.at[d - 1], gr2.at[d - 1], {"grp": z_peer(d)})
            for d in range(1, nz)
        ]
        gather_xy = {}

        def spread(d, zz):
            for k in range(1, nxy):
                gather_xy[d, k] = remote(
                    full.at[core, zz, xy], full.at[core, zz, xy],
                    gs1.at[d, k - 1], gr1.at[d, k - 1], row_id(xy_peer(k)),
                )

        spread(0, z)
        u_norm = jnp.sqrt(squares.finish() + FLOOR_SQ)
        filler(3)
        for d in range(1, nz):
            gather_z[d - 1].wait_recv()
            spread(d, z_peer(nz - d))
        filler(1)
        gather_core = []
        consume = consume(u_norm)
        for d in range(nz):
            zz = z_peer((nz - d) % nz)
            for k in range(1, nxy):
                gather_xy[d, k].wait_recv()
            gather_core.append(
                remote(full.at[core, zz], full.at[core, zz], gs0.at[d], gr0.at[d], core_id)
            )
            consume(core, zz)
            if d:
                gather_core[d - 1].wait_recv()
                consume(other, z_peer((nz - d + 1) % nz))
        gather_core[nz - 1].wait_recv()
        consume(other, z_peer(1 % nz))
        for copies in (core_copies, xy_copies, z_copies, gather_xy):
            for copy in copies.values():
                copy.wait_send()
        for copy in gather_z + gather_core:
            copy.wait_send()
        return u_norm

    live = (lax.broadcasted_iota(jnp.int32, (local, 1), 0) < count_ref[0]).astype(F32)

    load_b.wait()
    residue = live * b_ref[...].astype(F32)
    left_ref[...] = residue
    sq = jnp.sum(residue * residue, axis=0, keepdims=True)
    bt = residue.T.astype(BF16)
    load_other.wait()

    def first_product(half, s):
        start = pl.multiple_of((half * nz + s) * group, group)
        return jnp.dot(bt, a_ref[:, pl.ds(start, group)], preferred_element_type=F32).T

    block = 256
    todo = list(range(width // block))

    def form_c(times):
        if len(todo) == width // block:
            load_n.wait()
        for _ in range(times):
            if todo:
                at = todo.pop(0) * block
                value = live * jnp.dot(a_ref[...], n_ref[:, at : at + block], preferred_element_type=F32)
                c_ref[:, at : at + block] = value.astype(BF16)
                ct_ref[at : at + block, :] = value.T.astype(BF16)

    def later_product(half, s):
        start = pl.multiple_of((half * nz + s) * group, group)
        return jnp.dot(ct_ref[pl.ds(start, group), :], pb_ref[...], preferred_element_type=F32)

    def rows_of(half, s):
        return pl.ds(pl.multiple_of((half * nz + s) * group, group), group)

    def fold(raw):
        return jnp.sum((raw * raw).reshape(-1, 8, cols), axis=0)

    def norm_of(terms):
        total = sum(norms_ref[at] for at in range(terms))
        return jnp.sqrt(jnp.sum(total, axis=0, keepdims=True) + FLOOR_SQ)

    def pull_group(u_norm):
        pull_ref[...] = jnp.zeros_like(pull_ref)

        def consume(half, s):
            turned = flat(full[half, s]).T.astype(BF16)
            pull_ref[...] += jnp.dot(turned, n_ref[rows_of(half, s), :], preferred_element_type=F32)

        return consume

    def advance_group(turn, scale):
        def begin(u_norm):
            inverse = 1.0 / u_norm
            back = u_norm * scale
            acc_ref[...] = jnp.zeros_like(acc_ref)

            def consume(half, s):
                rows = rows_of(half, s)
                raw = flat(full[half, s]) * inverse - back * vecs_ref[turn, rows]
                vecs_ref[turn + 1, rows] = raw
                norms_ref[half * nz + s] = fold(raw)
                acc_ref[...] += jnp.dot(c_ref[:, rows], raw.astype(BF16), preferred_element_type=F32)

            return consume

        return begin

    u_norm = all_reduce(0, first_product, sq, form_c, pull_group)
    form_c(len(todo))
    inverse = 1.0 / u_norm
    acc = None
    for i, at in enumerate(range(0, width, block)):
        raw = pull_ref[:, at : at + block].T * inverse
        vecs_ref[0, at : at + block] = raw
        norms_ref[i] = fold(raw)
        term = jnp.dot(c_ref[:, at : at + block], raw.astype(BF16), preferred_element_type=F32)
        if i:
            acc_ref[...] += term
        else:
            acc_ref[...] = term
    v_norm = norm_of(width // block)
    scales = [1.0 / v_norm]
    phi_bar = u_norm
    rho_bar = v_norm
    start_norm = u_norm
    search = [jnp.ones((1, cols), F32)]
    coeffs = [jnp.zeros((1, cols), F32)]

    def project(v_norm, u_norm):
        residue = acc_ref[...] * (1.0 / v_norm) - left_ref[...] * (v_norm / u_norm)
        left_ref[...] = residue
        pb_ref[...] = residue.astype(BF16)
        return jnp.sum(residue * residue, axis=0, keepdims=True)

    for turn in range(ITERS - 1):
        sq = project(v_norm, u_norm)
        u_norm = all_reduce(
            turn + 1, later_product, sq, lambda times: None, advance_group(turn, scales[turn])
        )
        v_norm = norm_of(CORES * nz)
        scales.append(1.0 / v_norm)
        radius = jnp.sqrt(rho_bar * rho_bar + u_norm * u_norm)
        cosine = rho_bar / radius
        sine = u_norm / radius
        coupling = sine * v_norm
        rho_bar = -cosine * v_norm
        step = cosine * phi_bar / radius
        phi_bar = sine * phi_bar
        coeffs = [c + step * p for c, p in zip(coeffs, search)] + [jnp.zeros((1, cols), F32)]
        search = [-(coupling / radius) * p for p in search] + [jnp.ones((1, cols), F32)]

    squares = Squares(ITERS, project(v_norm, u_norm))
    squares.send_rows()
    coeffs = [c * scale for c, scale in zip(coeffs, scales)]
    search = [p * scale for p, scale in zip(search, scales)]
    for at in range(0, width, block):
        known = sum(c * vecs_ref[i, at : at + block] for i, c in enumerate(coeffs))
        along = sum(p * vecs_ref[i, at : at + block] for i, p in enumerate(search))
        flip_ref[:cols, at : at + block] = known.T
        flip_ref[cols:, at : at + block] = along.T
        w_ref[at : at + block, :cols] = known.astype(BF16)
        w_ref[at : at + block, cols:] = along.astype(BF16)

    def form_solution(first, last):
        for at in range(first, last, block):
            nw_ref[:, at : at + block] = jnp.dot(
                n_ref[at : at + block, :], w_ref[...], preferred_element_type=F32
            ).T

    squares.send_z()
    form_solution(0, width)
    u_norm = jnp.sqrt(squares.finish() + FLOOR_SQ)
    radius = jnp.sqrt(rho_bar * rho_bar + u_norm * u_norm)
    step = rho_bar / radius * phi_bar / radius
    ratio = u_norm / radius * phi_bar / start_norm
    shift = lax.rem(cols - z * own_cols, cols)
    ratio_ref[...] = pltpu.roll(jnp.broadcast_to(ratio, (8, cols)), shift, 1)[0:1, :own_cols]
    step_ref[...] = jnp.broadcast_to(step, (cols, cols)).T
    mine = pl.ds(pl.multiple_of(z * own_cols, own_cols), own_cols)
    mine_too = pl.ds(pl.multiple_of(cols + z * own_cols, own_cols), own_cols)
    step = step_ref[mine, :]
    for at in range(0, width, cols):
        span = slice(at, at + cols)
        coef_ref[:, span] = flip_ref[mine, span] + step * flip_ref[mine_too, span]
        sol_ref[:, span] = nw_ref[mine, span] + step * nw_ref[mine_too, span]


def shards(nrows, nz, matrix, right_side, precond, row_counts):
    local, width = matrix.shape
    cols = right_side.shape[1]
    nxy = nrows // CORES
    chunk = width // (nrows * nz)
    own = cols // nz
    turns = ITERS + 1
    vmem = pltpu.VMEM
    dma = pltpu.SemaphoreType.DMA
    sol, coef, ratio = pl.pallas_call(
        functools.partial(body, nrows, nz),
        out_shape=(
            jax.ShapeDtypeStruct((own, width), F32),
            jax.ShapeDtypeStruct((own, width), F32),
            jax.ShapeDtypeStruct((1, own), F32),
        ),
        in_specs=[
            pl.BlockSpec(memory_space=pltpu.SMEM),
            pl.BlockSpec(memory_space=pl.ANY),
            pl.BlockSpec(memory_space=pl.ANY),
            pl.BlockSpec(memory_space=pl.ANY),
        ],
        out_specs=[pl.BlockSpec(memory_space=vmem)] * 3,
        scratch_shapes=[
            vmem((local, width), BF16),
            vmem((local, cols), BF16),
            vmem((width, width), BF16),
            vmem((local, width), BF16),
            vmem((width, local), BF16),
            vmem((local, cols), F32),
            vmem((ITERS, width, cols), F32),
            vmem((local, cols), BF16),
            vmem((local, cols), F32),
            vmem((cols, width), F32),
            vmem((max(CORES * nz, width // 256), 8, cols), F32),
            vmem((width, 2 * cols), BF16),
            vmem((2 * cols, width), F32),
            vmem((2 * cols, width), F32),
            vmem((cols, cols), F32),
            vmem((nz, nxy, chunk, cols), BF16),
            vmem((nz, nxy, chunk, cols), BF16),
            vmem((nz, nxy, chunk, cols), F32),
            vmem((nz, nxy, chunk, cols), BF16),
            vmem((nz, nxy - 1, chunk, cols), BF16),
            vmem((nz - 1, chunk, cols), BF16),
            vmem((nz - 1, chunk, cols), BF16),
            vmem((CORES, nz, nxy, chunk, cols), BF16),
            vmem((turns, 2, 8, cols), F32),
            vmem((turns, nrows, 8, cols), F32),
            vmem((turns, nz, 8, cols), F32),
            dma((4,)),
            dma((nz,)), dma((nz,)),
            dma((nz, nxy - 1)), dma((nz, nxy - 1)),
            dma((nz - 1,)), dma((nz - 1,)),
            dma((nz - 1,)), dma((nz - 1,)),
            dma((nz, nxy - 1)), dma((nz, nxy - 1)),
            dma((nz,)), dma((nz,)),
            dma((turns, nrows - 1)), dma((turns, nrows - 1)),
            dma((turns, nz - 1)), dma((turns, nz - 1)),
        ],
        compiler_params=pltpu.CompilerParams(
            collective_id=0, has_side_effects=True, vmem_limit_bytes=60 * 1024 * 1024
        ),
    )(row_counts, matrix, right_side, precond)
    return (sol.T, coef.T, ratio[0])


def solution(mesh):
    return jax.shard_map(
        functools.partial(shards, mesh.shape["rows"], mesh.shape["grp"]),
        mesh=mesh,
        in_specs=(P(("rows", "grp"), None), P(("rows", "grp"), None), P(), P(("rows", "grp"))),
        out_specs=(P(None, "grp"), P(None, "grp"), P("grp")),
        check_vma=False,
    )
```

```python
import functools

import jax
import jax.numpy as jnp
from jax import lax
from jax.experimental import pallas as pl
from jax.experimental.pallas import tpu as pltpu
from jax.sharding import PartitionSpec as P

ITERS = 3
CORES = 2
FLOOR_SQ = 0.01
F32 = jnp.float32
BF16 = jnp.bfloat16
MESH = pl.DeviceIdType.MESH


def body(
    nrows, nz,
    count_ref, a_hbm, b_hbm, n_hbm,
    both_ref, ratio_ref,
    a_ref, b_ref, n_ref, c_ref, ct_ref, left_ref, vecs_ref, pb_ref, acc_ref, pull_ref, norms_ref,
    w_ref, flip_ref, nw_ref, step_ref,
    tx0, rx0, hbuf, tx1, rx1, tx2, rx2, full,
    sqtx, sqrx1, sqrx2,
    load_sem, s0, r0, s1, r1, s2, r2, gs2, gr2, gs1, gr1, gs0, gr0,
    qs1, qr1, qs2, qr2,
):
    row = lax.axis_index("rows")
    z = lax.axis_index("grp")
    core = lax.rem(row, CORES)
    xy = row // CORES
    other = 1 - core
    local, width = a_ref.shape
    cols = b_ref.shape[1]
    chunk = full.shape[3]
    nxy = nrows // CORES
    group = nxy * chunk
    own_cols = cols // nz

    def xy_peer(k):
        return lax.rem(xy + k, nxy)

    def z_peer(k):
        return lax.rem(z + k, nz)

    def row_id(at):
        return {"rows": at * CORES + core}

    core_id = {"rows": xy * CORES + other}

    def load_half(half, at):
        span = pl.ds(pl.multiple_of(half * (width // CORES), width // CORES), width // CORES)
        return pltpu.make_async_copy(a_hbm.at[:, span], a_ref.at[:, span], load_sem.at[at])

    load_b = pltpu.make_async_copy(b_hbm, b_ref, load_sem.at[3])
    load_other = load_half(other, 0)
    load_own = load_half(core, 1)
    load_n = pltpu.make_async_copy(n_hbm, n_ref, load_sem.at[2])
    load_b.start()
    load_other.start()
    load_own.start()

    barrier = pltpu.get_barrier_semaphore()
    for k in range(1, nrows):
        pl.semaphore_signal(barrier, inc=1, device_id={"rows": lax.rem(row + k, nrows)}, device_id_type=MESH)
    for k in range(1, nz):
        pl.semaphore_signal(barrier, inc=1, device_id={"grp": z_peer(k)}, device_id_type=MESH)

    def remote(src, dst, ssem, rsem, to):
        copy = pltpu.make_async_remote_copy(
            src_ref=src, dst_ref=dst, send_sem=ssem, recv_sem=rsem, device_id=to, device_id_type=MESH
        )
        copy.start()
        return copy

    def flat(value):
        return value.astype(F32).reshape(-1, cols)

    def pieces(value):
        return value.reshape(-1, chunk, cols).astype(BF16)

    class Squares:
        def __init__(self, turn, local_sq):
            self.turn = turn
            self.total = jnp.broadcast_to(local_sq, (8, cols))
            self.sent = []

        def send_rows(self):
            sqtx[self.turn, 0] = self.total
            sqrx1[self.turn, row] = self.total
            self.now = [
                remote(
                    sqtx.at[self.turn, 0], sqrx1.at[self.turn, row],
                    qs1.at[self.turn, k - 1], qr1.at[self.turn, k - 1],
                    {"rows": lax.rem(row + k, nrows)},
                )
                for k in range(1, nrows)
            ]

        def send_z(self):
            for copy in self.now:
                copy.wait_recv()
            self.sent += self.now
            self.total = sum(sqrx1[self.turn, at] for at in range(nrows))
            sqtx[self.turn, 1] = self.total
            sqrx2[self.turn, z] = self.total
            self.now = [
                remote(sqtx.at[self.turn, 1], sqrx2.at[self.turn, z], qs2.at[self.turn, k - 1], qr2.at[self.turn, k - 1], {"grp": z_peer(k)})
                for k in range(1, nz)
            ]

        def finish(self):
            for copy in self.now:
                copy.wait_recv()
            self.sent += self.now
            self.total = sum(sqrx2[self.turn, at] for at in range(nz))
            for copy in self.sent:
                copy.wait_send()
            return self.total[0:1]

    def all_reduce(turn, product, local_sq, filler, consume):
        order = list(range(1, nz)) + [0]
        sends = []
        core_copies = {}
        for d in order:
            s = z_peer(d)
            tx0[s] = pieces(product(other, s))
            if turn == 0 and d == order[0]:
                pl.semaphore_wait(barrier, nrows + nz - 2)
            core_copies[d] = remote(tx0.at[s], rx0.at[s], s0.at[d], r0.at[d], core_id)
        squares = Squares(turn, local_sq)
        squares.send_rows()
        if turn == 0:
            load_own.wait()
            load_n.start()
        for d in order:
            s = z_peer(d)
            hbuf[s] = product(core, s).reshape(nxy, chunk, cols)
        xy_copies = {}
        for d in order:
            s = z_peer(d)
            core_copies[d].wait_recv()
            total = hbuf[s] + rx0[s].astype(F32)
            hbuf[s] = total
            tx1[s] = total.astype(BF16)
            for k in range(1, nxy):
                at = xy_peer(k)
                xy_copies[d, k] = remote(
                    tx1.at[s, at], rx1.at[d, k - 1], s1.at[d, k - 1], r1.at[d, k - 1], row_id(at)
                )
        filler(2)
        z_copies = {}
        for d in order:
            s = z_peer(d)
            part = hbuf[s, xy]
            for k in range(1, nxy):
                xy_copies[d, k].wait_recv()
                part = part + rx1[d, k - 1].astype(F32)
            if d:
                tx2[d - 1] = part.astype(BF16)
                z_copies[d] = remote(
                    tx2.at[d - 1], rx2.at[d - 1], s2.at[d - 1], r2.at[d - 1], {"grp": s}
                )
        squares.send_z()
        filler(2)
        for d in range(1, nz):
            z_copies[d].wait_recv()
            part = part + rx2[d - 1].astype(F32)
        full[core, z, xy] = part.astype(BF16)
        gather_z = [
            remote(full.at[core, z, xy], full.at[core, z, xy], gs2.at[d - 1], gr2.at[d - 1], {"grp": z_peer(d)})
            for d in range(1, nz)
        ]
        gather_xy = {}

        def spread(d, zz):
            for k in range(1, nxy):
                gather_xy[d, k] = remote(
                    full.at[core, zz, xy], full.at[core, zz, xy],
                    gs1.at[d, k - 1], gr1.at[d, k - 1], row_id(xy_peer(k)),
                )

        spread(0, z)
        u_norm = jnp.sqrt(squares.finish() + FLOOR_SQ)
        filler(3)
        for d in range(1, nz):
            gather_z[d - 1].wait_recv()
            spread(d, z_peer(nz - d))
        filler(1)
        gather_core = []
        consume = consume(u_norm)
        for d in range(nz):
            zz = z_peer((nz - d) % nz)
            for k in range(1, nxy):
                gather_xy[d, k].wait_recv()
            gather_core.append(
                remote(full.at[core, zz], full.at[core, zz], gs0.at[d], gr0.at[d], core_id)
            )
            consume(core, zz)
            if d and turn:
                gather_core[d - 1].wait_recv()
                consume(other, z_peer((nz - d + 1) % nz))
        for d in range(nz - 1 if turn else 0, nz):
            gather_core[d].wait_recv()
            consume(other, z_peer((nz - d) % nz))
        for copies in (core_copies, xy_copies, z_copies, gather_xy):
            for copy in copies.values():
                copy.wait_send()
        for copy in gather_z + gather_core:
            copy.wait_send()
        return u_norm

    live = (lax.broadcasted_iota(jnp.int32, (local, 1), 0) < count_ref[0]).astype(F32)

    load_b.wait()
    residue = live * b_ref[...].astype(F32)
    left_ref[...] = residue
    sq = jnp.sum(residue * residue, axis=0, keepdims=True)
    bt = residue.T.astype(BF16)
    load_other.wait()

    def first_product(half, s):
        start = pl.multiple_of((half * nz + s) * group, group)
        return jnp.dot(bt, a_ref[:, pl.ds(start, group)], preferred_element_type=F32).T

    block = 256
    todo = list(range(width // block))

    def form_c(times):
        if len(todo) == width // block:
            load_n.wait()
        for _ in range(times):
            if todo:
                at = todo.pop(0) * block
                value = live * jnp.dot(a_ref[...], n_ref[:, at : at + block], preferred_element_type=F32)
                c_ref[:, at : at + block] = value.astype(BF16)
                ct_ref[at : at + block, :] = value.T.astype(BF16)

    def later_product(half, s):
        start = pl.multiple_of((half * nz + s) * group, group)
        return jnp.dot(ct_ref[pl.ds(start, group), :], pb_ref[...], preferred_element_type=F32)

    def rows_of(half, s):
        return pl.ds(pl.multiple_of((half * nz + s) * group, group), group)

    def fold(raw):
        return jnp.sum((raw * raw).reshape(-1, 8, cols), axis=0)

    def norm_of(terms):
        total = sum(norms_ref[at] for at in range(terms))
        return jnp.sqrt(jnp.sum(total, axis=0, keepdims=True) + FLOOR_SQ)

    def pull_group(u_norm):
        pull_ref[...] = jnp.zeros_like(pull_ref)

        def consume(half, s):
            turned = flat(full[half, s]).T.astype(BF16)
            pull_ref[...] += jnp.dot(turned, n_ref[rows_of(half, s), :], preferred_element_type=F32)

        return consume

    def advance_group(turn, scale):
        def begin(u_norm):
            inverse = 1.0 / u_norm
            back = u_norm * scale
            acc_ref[...] = jnp.zeros_like(acc_ref)

            def consume(half, s):
                rows = rows_of(half, s)
                raw = flat(full[half, s]) * inverse - back * vecs_ref[turn, rows]
                vecs_ref[turn + 1, rows] = raw
                norms_ref[half * nz + s] = fold(raw)
                acc_ref[...] += jnp.dot(c_ref[:, rows], raw.astype(BF16), preferred_element_type=F32)

            return consume

        return begin

    u_norm = all_reduce(0, first_product, sq, form_c, pull_group)
    form_c(len(todo))
    inverse = 1.0 / u_norm
    acc = None
    for i, at in enumerate(range(0, width, block)):
        raw = pull_ref[:, at : at + block].T * inverse
        vecs_ref[0, at : at + block] = raw
        norms_ref[i] = fold(raw)
        term = jnp.dot(c_ref[:, at : at + block], raw.astype(BF16), preferred_element_type=F32)
        if i:
            acc_ref[...] += term
        else:
            acc_ref[...] = term
    v_norm = norm_of(width // block)
    scales = [1.0 / v_norm]
    phi_bar = u_norm
    rho_bar = v_norm
    start_norm = u_norm
    search = [jnp.ones((1, cols), F32)]
    coeffs = [jnp.zeros((1, cols), F32)]

    def project(v_norm, u_norm):
        residue = acc_ref[...] * (1.0 / v_norm) - left_ref[...] * (v_norm / u_norm)
        left_ref[...] = residue
        pb_ref[...] = residue.astype(BF16)
        return jnp.sum(residue * residue, axis=0, keepdims=True)

    for turn in range(ITERS - 1):
        sq = project(v_norm, u_norm)
        u_norm = all_reduce(
            turn + 1, later_product, sq, lambda times: None, advance_group(turn, scales[turn])
        )
        v_norm = norm_of(CORES * nz)
        scales.append(1.0 / v_norm)
        radius = jnp.sqrt(rho_bar * rho_bar + u_norm * u_norm)
        cosine = rho_bar / radius
        sine = u_norm / radius
        coupling = sine * v_norm
        rho_bar = -cosine * v_norm
        step = cosine * phi_bar / radius
        phi_bar = sine * phi_bar
        coeffs = [c + step * p for c, p in zip(coeffs, search)] + [jnp.zeros((1, cols), F32)]
        search = [-(coupling / radius) * p for p in search] + [jnp.ones((1, cols), F32)]

    squares = Squares(ITERS, project(v_norm, u_norm))
    squares.send_rows()
    coeffs = [c * scale for c, scale in zip(coeffs, scales)]
    search = [p * scale for p, scale in zip(search, scales)]
    for at in range(0, width, block):
        known = sum(c * vecs_ref[i, at : at + block] for i, c in enumerate(coeffs))
        along = sum(p * vecs_ref[i, at : at + block] for i, p in enumerate(search))
        flip_ref[:cols, at : at + block] = known.T
        flip_ref[cols:, at : at + block] = along.T
        w_ref[at : at + block, :cols] = known.astype(BF16)
        w_ref[at : at + block, cols:] = along.astype(BF16)

    def form_solution(first, last):
        for at in range(first, last, block):
            nw_ref[:, at : at + block] = jnp.dot(
                n_ref[at : at + block, :], w_ref[...], preferred_element_type=F32
            ).T

    squares.send_z()
    form_solution(0, width)
    u_norm = jnp.sqrt(squares.finish() + FLOOR_SQ)
    radius = jnp.sqrt(rho_bar * rho_bar + u_norm * u_norm)
    step = rho_bar / radius * phi_bar / radius
    ratio = u_norm / radius * phi_bar / start_norm
    shift = lax.rem(cols - z * own_cols, cols)
    ratio_ref[...] = pltpu.roll(jnp.broadcast_to(ratio, (8, cols)), shift, 1)[0:1, :own_cols]
    step_ref[...] = jnp.broadcast_to(step, (cols, cols)).T
    mine = pl.ds(pl.multiple_of(z * own_cols, own_cols), own_cols)
    mine_too = pl.ds(pl.multiple_of(cols + z * own_cols, own_cols), own_cols)
    step = step_ref[mine, :]
    for at in range(0, width, cols):
        span = slice(at, at + cols)
        both_ref[own_cols:, span] = flip_ref[mine, span] + step * flip_ref[mine_too, span]
        both_ref[:own_cols, span] = nw_ref[mine, span] + step * nw_ref[mine_too, span]


def hand_over(both_hbm, ratio_in, sol_hbm, coef_hbm, ratio_out, held, in_sem, out_sem):
    own = sol_hbm.shape[0]
    halves = [pl.ds(0, own), pl.ds(own, own)]
    inward = [
        pltpu.make_async_copy(both_hbm.at[half], held.at[half], in_sem.at[i]) for i, half in enumerate(halves)
    ]
    outward = [
        pltpu.make_async_copy(held.at[half], to, out_sem.at[i])
        for i, (half, to) in enumerate(zip(halves, (sol_hbm, coef_hbm)))
    ]
    for copy in inward:
        copy.start()
    ratio_out[...] = ratio_in[...]
    for first, second in zip(inward, outward):
        first.wait()
        second.start()
    for copy in outward:
        copy.wait()


def shards(nrows, nz, matrix, right_side, precond, row_counts):
    local, width = matrix.shape
    cols = right_side.shape[1]
    nxy = nrows // CORES
    chunk = width // (nrows * nz)
    own = cols // nz
    turns = ITERS + 1
    vmem = pltpu.VMEM
    dma = pltpu.SemaphoreType.DMA
    both, ratio = pl.pallas_call(
        functools.partial(body, nrows, nz),
        out_shape=(
            jax.ShapeDtypeStruct((2 * own, width), F32),
            jax.ShapeDtypeStruct((1, own), F32),
        ),
        in_specs=[
            pl.BlockSpec(memory_space=pltpu.SMEM),
            pl.BlockSpec(memory_space=pl.ANY),
            pl.BlockSpec(memory_space=pl.ANY),
            pl.BlockSpec(memory_space=pl.ANY),
        ],
        out_specs=[pl.BlockSpec(memory_space=vmem)] * 2,
        scratch_shapes=[
            vmem((local, width), BF16),
            vmem((local, cols), BF16),
            vmem((width, width), BF16),
            vmem((local, width), BF16),
            vmem((width, local), BF16),
            vmem((local, cols), F32),
            vmem((ITERS, width, cols), F32),
            vmem((local, cols), BF16),
            vmem((local, cols), F32),
            vmem((cols, width), F32),
            vmem((max(CORES * nz, width // 256), 8, cols), F32),
            vmem((width, 2 * cols), BF16),
            vmem((2 * cols, width), F32),
            vmem((2 * cols, width), F32),
            vmem((cols, cols), F32),
            vmem((nz, nxy, chunk, cols), BF16),
            vmem((nz, nxy, chunk, cols), BF16),
            vmem((nz, nxy, chunk, cols), F32),
            vmem((nz, nxy, chunk, cols), BF16),
            vmem((nz, nxy - 1, chunk, cols), BF16),
            vmem((nz - 1, chunk, cols), BF16),
            vmem((nz - 1, chunk, cols), BF16),
            vmem((CORES, nz, nxy, chunk, cols), BF16),
            vmem((turns, 2, 8, cols), F32),
            vmem((turns, nrows, 8, cols), F32),
            vmem((turns, nz, 8, cols), F32),
            dma((4,)),
            dma((nz,)), dma((nz,)),
            dma((nz, nxy - 1)), dma((nz, nxy - 1)),
            dma((nz - 1,)), dma((nz - 1,)),
            dma((nz - 1,)), dma((nz - 1,)),
            dma((nz, nxy - 1)), dma((nz, nxy - 1)),
            dma((nz,)), dma((nz,)),
            dma((turns, nrows - 1)), dma((turns, nrows - 1)),
            dma((turns, nz - 1)), dma((turns, nz - 1)),
        ],
        compiler_params=pltpu.CompilerParams(
            collective_id=0, has_side_effects=True, vmem_limit_bytes=60 * 1024 * 1024
        ),
    )(row_counts, matrix, right_side, precond)
    sol, coef, ratio = pl.pallas_call(
        hand_over,
        out_shape=(
            jax.ShapeDtypeStruct((own, width), F32),
            jax.ShapeDtypeStruct((own, width), F32),
            jax.ShapeDtypeStruct((1, own), F32),
        ),
        in_specs=[pl.BlockSpec(memory_space=pl.ANY), pl.BlockSpec(memory_space=vmem)],
        out_specs=[
            pl.BlockSpec(memory_space=pl.ANY),
            pl.BlockSpec(memory_space=pl.ANY),
            pl.BlockSpec(memory_space=vmem),
        ],
        scratch_shapes=[vmem((2 * own, width), F32), dma((2,)), dma((2,))],
        compiler_params=pltpu.CompilerParams(vmem_limit_bytes=60 * 1024 * 1024),
    )(both, ratio)
    return (sol.T, coef.T, ratio[0])


def solution(mesh):
    return jax.shard_map(
        functools.partial(shards, mesh.shape["rows"], mesh.shape["grp"]),
        mesh=mesh,
        in_specs=(P(("rows", "grp"), None), P(("rows", "grp"), None), P(), P(("rows", "grp"))),
        out_specs=(P(None, "grp"), P(None, "grp"), P("grp")),
        check_vma=False,
    )
```
